32 devices in a mesh: groups: 2 (over x), seq: 4 (over y, core), dp: 4 (over z).
Axes of the slice: x: 2, y: 2, z: 4, core: 2. Of those that a mesh axis runs over, the one named last changes fastest.
Arguments:
- resid: bfloat16 [8, 256, 2048], P(('groups', 'dp'), 'seq'), parts along dimension 0, may hold values from -6 to 6
- queries_keys: bfloat16 [2, 8, 256, 2048], P(None, ('groups', 'dp'), 'seq'), parts along dimension 1, may hold values from -20 to 20
- values: bfloat16 [8, 256, 2048], P(('groups', 'dp'), 'seq'), parts along dimension 0, may hold values from -6 to 6
- doc_ids: int32 [8, 256], P(('groups', 'dp')), parts along dimension 0, may hold values from 0 to 5, never falling along the last dimension, each value on 1 to 128 neighbouring positions
- out_weight: bfloat16 [2048, 2048], P(None, 'dp'), may hold values from -0.125 to 0.125
- norm_gain: float32 [2048], replicated, may hold values from 0.5 to 1.5
- expert_ids: int32 [8, 256, 4], P(('groups', 'dp'), 'seq'), parts along dimension 0, may hold values from 0 to 31, all different within a row; in each aligned block of 64 rows (0 to 63, 64 to 127, ..., all dimensions but the last counted through in order) at most 10 rows name the same one
- gate_vals: float32 [8, 256, 4], P(('groups', 'dp'), 'seq'), parts along dimension 0, may hold values from 0.05 to 0.6
- expert_gate: bfloat16 [128, 2048, 352], P(('seq', 'dp')), may hold values from -0.125 to 0.125
- expert_up: bfloat16 [128, 2048, 352], P(('seq', 'dp')), may hold values from -0.125 to 0.125
- expert_down: bfloat16 [128, 352, 2048], P(('seq', 'dp')), may hold values from -0.15625 to 0.15625
- shared_gate: bfloat16 [2048, 2816], P(None, 'dp'), may hold values from -0.125 to 0.125
- shared_up: bfloat16 [2048, 2816], P(None, 'dp'), may hold values from -0.125 to 0.125
- shared_down: bfloat16 [2816, 2048], P('dp'), may hold values from -0.109375 to 0.109375
- shared_score: bfloat16 [2048], replicated, may hold values from -0.125 to 0.125
Outputs:
- layer_out: bfloat16 [8, 256, 2048], P(('groups', 'dp'), 'seq'), parts along dimension 0
The draws below stay inside these ranges and needn't reach their ends.
There are 2 independent parts, one for each index of `groups`. The reference program is written for one: setup_inputs(seed, part) draws one part's arguments, and reference() takes and returns one part's arrays. A program takes and returns all parts, laid end to end along the dimension named above; an argument that names none is the same for every part. Nothing has to cross between parts.
Inputs may be any that keep to these rules, and one draw needn't show every extreme that they name: `doc_ids`: document numbers never fall along a sequence; each document holds 1 to 128 positions. `expert_ids`: each token names 4 different experts; among the rows of one device no expert is named more than 10 times.
All inputs are finite; a program needn't handle non-finite values.
Results may differ from the reference program's by a relative error of at most 0.01.
Values may be sent and summed in bfloat16 or wider, within the bound.
A program may use at most 128 MiB of HBM per device.

```python
import math
import jax
import jax.numpy as jnp
import numpy as np
from jax import lax

HEADS = 16
HD = 128
D = 2048
EXPERTS = 32
TOPK = 4
FF_E = 1408
SPLIT = 4
PIECES = 128
PIECE_FF = 352
SH_FF = 2816
TOK_DEV = 64
CAP = 10
LENGTH = 256
SEQS = 4
N_DP = 4


def draw_queries_keys(key, part):
    baseline = jnp.clip(jax.random.normal(key, (2, SEQS, LENGTH, D), jnp.float32), -6.0, 6.0)
    return baseline.astype(jnp.bfloat16)


def block_levels(rng, extent, pieces, smallest, largest):
    factor_of, own = 1.0, jax.random.fold_in(rng, 6)
    for dim, shards_of in pieces:
        heights = jnp.exp(jax.random.uniform(jax.random.fold_in(own, dim), (shards_of,), jnp.float32, smallest / len(pieces), largest / len(pieces)))
        factor_of = factor_of * jnp.repeat(heights, extent[dim] // shards_of).reshape([-1 if axis == dim else 1 for axis in range(len(extent))])
    return factor_of


def length_profile(number_of, total, reach, skew):
    loads = [(1 << 20) // math.isqrt(grade ** skew) + 1 for grade in range(2, number_of + 1)]
    rest, counts = total - reach - (number_of - 1), [1] * (number_of - 1)
    while rest > 0:
        candidates = [i for i in range(number_of - 1) if counts[i] < reach]
        mass, left = sum([loads[i] for i in candidates]), rest
        for i in candidates:
            addition = min(reach - counts[i], max(1, left * loads[i] // mass), rest)
            counts[i] = counts[i] + addition
            rest = rest - addition
    return np.array([reach] + counts)


def uneven_parts(rng, number_of, total, limit, slope):
    if number_of == 2:
        one = jax.random.randint(rng, (), max(1, total - limit), min(limit, total - 1) + 1)
        return jnp.stack([one, total - one])
    lengths = jnp.asarray(length_profile(number_of, total, limit, slope), jnp.int32)
    couples = (number_of - 1) // 2
    giver, taker = lengths[1:1 + 2 * couples:2], lengths[2:2 + 2 * couples:2]
    margin = jnp.minimum(giver - 1, limit - taker)
    moved = jax.random.randint(jax.random.fold_in(rng, 1), (couples,), 0, 1 << 20) % (margin + 1)
    lengths = lengths.at[1:1 + 2 * couples:2].set(giver - moved).at[2:2 + 2 * couples:2].set(taker + moved)
    return lengths[jax.random.permutation(jax.random.fold_in(rng, 2), number_of)]


def assign_block(own_key, own, number, rows, count, top, bound, skew):
    ranking = jax.random.permutation(own_key, count)
    heavy_load, common = shares(count, rows * top, bound, skew, True), shares(count, rows * top, bound, skew, False)
    places = jnp.arange(count)

    def named(lengths, turn):
        used = int((lengths > 0).sum())
        fixed = max(1, used // 4)
        moved = fixed + (places - fixed + turn * (used - fixed)) % max(1, count - fixed)
        return jnp.zeros((count,), jnp.int32).at[ranking[jnp.where(places < fixed, places, moved)]].set(jnp.asarray(lengths, jnp.int32))

    lengths = jnp.where(number % 4 == 0, named(heavy_load, number // 4), named(common, number - number // 4 - 1))
    mixed = jax.random.permutation(jax.random.fold_in(own, 3), count)
    giver, sink = mixed[0:count // 2 * 2:2], mixed[1:count // 2 * 2:2]
    room = jnp.minimum(lengths[giver] - 1, bound - lengths[sink]) // 2
    room = jnp.where((giver == ranking[0]) | (sink == ranking[0]) | (lengths[sink] == 0), 0, jnp.maximum(room, 0))
    moved = jax.random.randint(jax.random.fold_in(own, 4), (count // 2,), 0, 1 << 20) % (room + 1)
    lengths = lengths.at[giver].add(-moved).at[sink].add(moved)
    labels = jnp.searchsorted(jnp.cumsum(lengths), jnp.arange(rows * top), side="right").astype(jnp.int32)
    grid = labels.reshape(top, rows).T
    grid = grid[jax.random.permutation(jax.random.fold_in(own, 1), rows)]
    turn = jax.random.randint(jax.random.fold_in(own, 2), (rows, 1), 0, top)
    return jnp.take_along_axis(grid, (jnp.arange(top)[None, :] + turn) % top, axis=1)


def shares(number_of, total, bound, lean, full):
    weights = [(1 << 20) // math.isqrt(grade ** lean) + 1 for grade in range(1, number_of + 1)]
    largest = bound if full else min(bound, max(-(-total // number_of), total * weights[0] // sum(weights)))
    least = 1 if total - largest >= number_of - 1 else 0
    counts, rest = [largest] + [least] * (number_of - 1), total - largest - least * (number_of - 1)
    while rest > 0:
        free = [i for i in range(1, number_of) if counts[i] < largest] or [i for i in range(1, number_of) if counts[i] < bound]
        whole, budget = sum([weights[i] for i in free]), rest
        for i in free:
            more = min(bound - counts[i], max(1, budget * weights[i] // whole), rest)
            counts[i] = counts[i] + more
            rest = rest - more
    return np.array(counts)


def bell_draw(own_key, shape, scale, most, pieces=(), kind=jnp.bfloat16):
    gain = block_levels(own_key, shape, pieces, -0.22, 0.18) if pieces else 1.0
    values = jax.random.normal(own_key, shape, jnp.float32) * scale * gain
    return jnp.minimum(jnp.maximum(values, -most), most).astype(kind)


def setup_inputs(seed: int = 0, part: int = 0) -> dict:
    key_of = jax.random.split(jax.random.key(seed), 16)
    part_splits = jax.random.split(jax.random.fold_in(key_of[15], part), 16)
    resid = bell_draw(part_splits[0], (SEQS, LENGTH, D), 1.0, 6.0, ((0, 4), (1, 4)))
    queries_keys = draw_queries_keys(jax.random.fold_in(jax.random.fold_in(key_of[15], part), 71), part)
    values = bell_draw(part_splits[2], (SEQS, LENGTH, D), 1.0, 6.0, ((0, 4), (1, 4)))
    doc_ids = jax.vmap(lambda own: jnp.searchsorted(jnp.cumsum(uneven_parts(own, 6, LENGTH, LENGTH // 2, 1)), jnp.arange(LENGTH), side="right"))(jax.random.split(part_splits[3], SEQS)).reshape((SEQS, LENGTH)).astype(jnp.int32)
    out_weight = bell_draw(key_of[4], (D, D), D ** -0.5, 0.125, ((1, 4),))
    norm_gain = jnp.clip(1.0 + 0.1 * jax.random.normal(key_of[5], (D,), jnp.float32), 0.5, 1.5)
    expert_ids_keys = jax.random.split(jax.random.fold_in(part_splits[6], 1), SEQS * LENGTH // TOK_DEV)
    expert_ids_turns = jax.random.permutation(jax.random.fold_in(part_splits[6], 3), SEQS * LENGTH // TOK_DEV)
    expert_ids = jax.vmap(lambda own, number: assign_block(jax.random.fold_in(part_splits[6], 2), own, number, TOK_DEV, EXPERTS, TOPK, CAP, 2))(expert_ids_keys, expert_ids_turns).reshape((SEQS, LENGTH, TOPK))
    gate_vals = jnp.clip(jnp.exp(math.log(0.6) - 2.4849067 * jax.random.uniform(part_splits[7], (SEQS, LENGTH, TOPK), jnp.float32) ** block_levels(part_splits[7], (SEQS, LENGTH, TOPK), ((0, 4), (1, 4)), -0.2, 0.2)), 0.05, 0.6)
    expert_gate = bell_draw(key_of[8], (PIECES, D, PIECE_FF), D ** -0.5, 0.125, ((0, 16),))
    expert_up = bell_draw(key_of[9], (PIECES, D, PIECE_FF), D ** -0.5, 0.125, ((0, 16),))
    expert_down = bell_draw(key_of[10], (PIECES, PIECE_FF, D), FF_E ** -0.5, 0.15625, ((0, 16),))
    shared_gate = bell_draw(key_of[11], (D, SH_FF), D ** -0.5, 0.125, ((1, 4),))
    shared_up = bell_draw(key_of[12], (D, SH_FF), D ** -0.5, 0.125, ((1, 4),))
    shared_down = bell_draw(key_of[13], (SH_FF, D), SH_FF ** -0.5, 0.109375, ((0, 4),))
    shared_score = bell_draw(key_of[14], (D,), D ** -0.5, 0.125)
    return dict(resid=resid, queries_keys=queries_keys, values=values, doc_ids=doc_ids, out_weight=out_weight, norm_gain=norm_gain, expert_ids=expert_ids, gate_vals=gate_vals, expert_gate=expert_gate, expert_up=expert_up, expert_down=expert_down, shared_gate=shared_gate, shared_up=shared_up, shared_down=shared_down, shared_score=shared_score)


norm_eps = 1e-06

def slot_numbers(routes):
    flat_routes = routes.reshape(routes.shape[:-2] + (-1,))
    matches = (flat_routes[..., None] == jnp.arange(EXPERTS, dtype=jnp.int32)).astype(jnp.int32)
    ranked = lax.optimization_barrier(jnp.sum(matches * (jnp.cumsum(matches, axis=-2) - 1), axis=-1))
    return (flat_routes * CAP + ranked).reshape(routes.shape).astype(jnp.int32)

def reference(resid, queries_keys, values, doc_ids, out_weight, norm_gain, expert_ids, gate_vals, expert_gate, expert_up, expert_down, shared_gate, shared_up, shared_down, shared_score):
    score_scale = 1.0 / math.sqrt(HD)
    positions = jnp.arange(LENGTH, dtype=jnp.int32)
    causal = positions[:, None] >= positions[None, :]

    def attend_sequence(inputs):
        pair_rows, value_rows, documents = inputs
        queries = pair_rows[0].astype(jnp.float32).reshape(LENGTH, HEADS, HD)
        key_rows = pair_rows[1].astype(jnp.float32).reshape(LENGTH, HEADS, HD)
        value_heads = value_rows.astype(jnp.float32).reshape(LENGTH, HEADS, HD)
        scores = jnp.einsum('qhd,khd->hqk', queries, key_rows) * score_scale
        allowed = causal & (documents[:, None] == documents[None, :])
        scores = jnp.where(allowed[None], scores, -1e+30)
        row_max = lax.optimization_barrier(jnp.max(scores, axis=-1, keepdims=True))
        lifted = jnp.exp(scores - row_max)
        weights = (lifted / lax.optimization_barrier(jnp.sum(lifted, axis=-1, keepdims=True))).astype(jnp.bfloat16)
        attended = jnp.einsum('hqk,khd->qhd', weights.astype(jnp.float32), value_heads).astype(jnp.bfloat16)
        return jnp.dot(attended.reshape(LENGTH, D), out_weight, preferred_element_type=jnp.float32).astype(jnp.bfloat16)
    projected = lax.map(attend_sequence, (jnp.moveaxis(queries_keys, 1, 0), values, doc_ids))
    residual = (resid.astype(jnp.float32) + projected.astype(jnp.float32)).astype(jnp.bfloat16)
    stream = residual.astype(jnp.float32)
    normed = (stream * lax.rsqrt(lax.optimization_barrier(jnp.mean(stream * stream, axis=-1, keepdims=True)) + norm_eps) * norm_gain).astype(jnp.bfloat16)
    shared_width = SH_FF // N_DP
    down_blocks = shared_down.astype(jnp.float32).reshape(N_DP, shared_width, D)

    def shared_sequence(row_block):
        gate_act = jnp.dot(row_block, shared_gate, preferred_element_type=jnp.float32)
        up_act = jnp.dot(row_block, shared_up, preferred_element_type=jnp.float32)
        hidden = (jax.nn.silu(gate_act) * up_act).astype(jnp.bfloat16)
        partial_sums = jnp.einsum('lnf,nfd->nld', hidden.astype(jnp.float32).reshape(-1, N_DP, shared_width), down_blocks)
        partial_sums = lax.optimization_barrier(partial_sums.astype(jnp.bfloat16)).astype(jnp.float32)
        return lax.optimization_barrier(jnp.sum(partial_sums, axis=0))
    shared_out = lax.map(shared_sequence, normed).reshape(-1, D)
    flat_rows = normed.reshape(-1, D)
    token_count = flat_rows.shape[0]
    share_weight = jax.nn.sigmoid(jnp.dot(flat_rows, shared_score, preferred_element_type=jnp.float32))
    blocks = token_count // TOK_DEV
    routes = expert_ids.reshape(blocks, TOK_DEV, TOPK).astype(jnp.int32)
    slot_ids = slot_numbers(routes)
    ranked = slot_ids - routes * CAP
    block_ids = jnp.arange(blocks, dtype=jnp.int32)[:, None, None]
    token_ids = block_ids * TOK_DEV + jnp.arange(TOK_DEV, dtype=jnp.int32)[None, :, None] + jnp.zeros_like(routes)
    row_slots = (block_ids * CAP + ranked).astype(jnp.int32)
    row_table = jnp.full((EXPERTS, blocks * CAP), token_count, jnp.int32).at[routes, row_slots].set(token_ids.astype(jnp.int32))
    gate_table = jnp.zeros((EXPERTS, blocks * CAP), jnp.float32).at[routes, row_slots].set(gate_vals.reshape(blocks, TOK_DEV, TOPK).astype(jnp.float32))
    padded = jnp.concatenate([flat_rows, jnp.zeros((1, D), jnp.bfloat16)], axis=0)
    gate_pieces = expert_gate.reshape(EXPERTS, SPLIT, D, PIECE_FF)
    up_pieces = expert_up.reshape(EXPERTS, SPLIT, D, PIECE_FF)
    down_pieces = expert_down.reshape(EXPERTS, SPLIT, PIECE_FF, D)

    def one_expert(running, inputs):
        index_rows, weight_rows, gate_matrix, up_matrix, down_matrix = inputs
        picked = padded[index_rows].astype(jnp.float32)
        gate_act = jnp.einsum('rd,sdf->srf', picked, gate_matrix.astype(jnp.float32))
        up_act = jnp.einsum('rd,sdf->srf', picked, up_matrix.astype(jnp.float32))
        hidden = (jax.nn.silu(gate_act) * up_act).astype(jnp.bfloat16)
        partial_sums = jnp.einsum('srf,sfd->srd', hidden.astype(jnp.float32), down_matrix.astype(jnp.float32))
        partial_sums = lax.optimization_barrier(partial_sums.astype(jnp.bfloat16)).astype(jnp.float32)
        output = lax.optimization_barrier(jnp.sum(partial_sums, axis=0))
        running = running.at[index_rows].add(weight_rows[:, None] * output)
        return (running, None)
    routed, unused = lax.scan(one_expert, jnp.zeros((token_count + 1, D), jnp.float32), (row_table, gate_table, gate_pieces, up_pieces, down_pieces))
    routed = routed[:token_count]
    layer_out = residual.reshape(-1, D).astype(jnp.float32) + routed + share_weight[:, None] * shared_out
    return layer_out.astype(jnp.bfloat16).reshape(SEQS, LENGTH, D)
```

```python
import math

import jax
import jax.numpy as jnp
from jax import lax
from jax.sharding import PartitionSpec as P

HD = 128
EXPERTS = 32
TOPK = 4
SPLIT = 4
CAP = 10


norm_eps = 1e-06


def slot_numbers(routes):
    flat_routes = routes.reshape(routes.shape[:-2] + (-1,))
    matches = (flat_routes[..., None] == jnp.arange(EXPERTS, dtype=jnp.int32)).astype(jnp.int32)
    ranked = jnp.sum(matches * (jnp.cumsum(matches, axis=-2) - 1), axis=-1)
    return (flat_routes * CAP + ranked).reshape(routes.shape)


def attend_heads(queries, key_rows, value_rows, documents):
    score_scale = 1.0 / math.sqrt(queries.shape[-1])
    scores = (
        jnp.einsum("qhd,khd->hqk", queries, key_rows, preferred_element_type=jnp.float32)
        * score_scale
    )
    positions = jnp.arange(queries.shape[0], dtype=jnp.int32)
    allowed = (positions[:, None] >= positions[None, :]) & (
        documents[:, None] == documents[None, :]
    )
    scores = jnp.where(allowed[None], scores, -1e30)
    row_max = jnp.max(scores, axis=-1, keepdims=True)
    lifted = jnp.exp(scores - row_max)
    weights = (lifted / jnp.sum(lifted, axis=-1, keepdims=True)).astype(jnp.bfloat16)
    return jnp.einsum(
        "hqk,khd->qhd", weights, value_rows, preferred_element_type=jnp.float32
    ).astype(jnp.bfloat16)


def piece_block(row_block, gate_matrix, up_matrix, down_matrix):
    gate_act = jnp.einsum(
        "npcd,pdf->npcf", row_block, gate_matrix, preferred_element_type=jnp.float32
    )
    up_act = jnp.einsum("npcd,pdf->npcf", row_block, up_matrix, preferred_element_type=jnp.float32)
    hidden = (jax.nn.silu(gate_act) * up_act).astype(jnp.bfloat16)
    return jnp.einsum(
        "npcf,pfd->npcd", hidden, down_matrix, preferred_element_type=jnp.float32
    ).astype(jnp.bfloat16)


def shared_block(row_block, gate_matrix, up_matrix, down_matrix):
    gate_act = jnp.dot(row_block, gate_matrix, preferred_element_type=jnp.float32)
    up_act = jnp.dot(row_block, up_matrix, preferred_element_type=jnp.float32)
    hidden = (jax.nn.silu(gate_act) * up_act).astype(jnp.bfloat16)
    return jnp.dot(hidden, down_matrix, preferred_element_type=jnp.float32)


def gathered_layer(residual, normed, expert_ids, gate_vals, gate, up, down, shared, score):
    everyone = ("seq", "dp")
    seq_count, batch_count = lax.axis_size("seq"), lax.axis_size("dp")
    devices = seq_count * batch_count
    tokens, width = normed.shape
    own_experts = gate.shape[0] // SPLIT
    room = devices * CAP
    table = jnp.concatenate([expert_ids[0].astype(jnp.float32), gate_vals[0]], axis=1)
    table = lax.all_gather(table, everyone, axis=0, tiled=True)
    me = lax.axis_index("seq") * batch_count + lax.axis_index("dp")
    mine = (me * own_experts + jnp.arange(own_experts)).astype(jnp.float32)
    named = (table[:, :TOPK, None] == mine).astype(jnp.float32)
    weight = jnp.sum(named * table[:, TOPK:, None], axis=1)
    named = jnp.sum(named, axis=1)
    total = devices * tokens
    order = jnp.arange(total)
    before = (order[None, :] < order[:, None]).astype(jnp.bfloat16)
    rank = jnp.dot(before, named.astype(jnp.bfloat16), preferred_element_type=jnp.float32)
    spot = jnp.where(named > 0, rank, -1.0)
    pick = spot.T[:, None, :] == jnp.arange(room, dtype=jnp.float32)[None, :, None]
    slot_gate = jnp.sum(jnp.where(pick, weight.T[:, None, :], 0.0), axis=-1)
    pick = pick.astype(jnp.bfloat16).reshape(own_experts * room, total)

    pool = lax.all_gather(normed, everyone, axis=0, tiled=True)
    rows = jnp.dot(pick, pool, preferred_element_type=jnp.float32).astype(jnp.bfloat16)
    rows = rows.reshape(own_experts, room, width)
    gate = gate.reshape((own_experts, SPLIT) + gate.shape[1:])
    up = up.reshape((own_experts, SPLIT) + up.shape[1:])
    down = down.reshape((own_experts, SPLIT) + down.shape[1:])
    gate_act = jnp.einsum("ecd,ebdf->ebcf", rows, gate, preferred_element_type=jnp.float32)
    up_act = jnp.einsum("ecd,ebdf->ebcf", rows, up, preferred_element_type=jnp.float32)
    hidden = (jax.nn.silu(gate_act) * up_act).astype(jnp.bfloat16)
    expert_out = jnp.einsum("ebcf,ebfd->ecd", hidden, down, preferred_element_type=jnp.float32)
    expert_out = (expert_out * slot_gate[..., None]).astype(jnp.bfloat16)
    partial = lax.dot_general(
        pick,
        expert_out.reshape(own_experts * room, width),
        (((0,), (0,)), ((), ())),
        preferred_element_type=jnp.float32,
    ).reshape(seq_count, batch_count * tokens, width)
    s = lax.axis_index("seq")
    line = lax.dynamic_slice_in_dim(pool, s * batch_count * tokens, batch_count * tokens)
    share_weight = jax.nn.sigmoid(jnp.dot(line, score, preferred_element_type=jnp.float32))
    shared_part = shared_block(line, *shared) * share_weight[:, None]
    here = (jnp.arange(seq_count) == s)[:, None, None]
    partial = jnp.where(here, partial + shared_part[None], partial).astype(jnp.bfloat16)
    summed = lax.psum_scatter(
        partial.reshape(total, width), everyone, scatter_dimension=0, tiled=True
    )
    out = residual.astype(jnp.float32) + summed.astype(jnp.float32)
    return out.astype(jnp.bfloat16)[None]


def body(
    resid,
    queries_keys,
    values,
    doc_ids,
    out_weight,
    norm_gain,
    expert_ids,
    gate_vals,
    expert_gate,
    expert_up,
    expert_down,
    shared_gate,
    shared_up,
    shared_down,
    shared_score,
):
    seq_count = lax.axis_size("seq")
    batch_count = lax.axis_size("dp")
    tokens = resid.shape[1]
    model_width = resid.shape[2]
    local_heads = model_width // HD // seq_count
    paired = queries_keys.reshape(2, tokens, seq_count, local_heads, HD)
    valued = values.reshape(1, tokens, seq_count, local_heads, HD)
    documents = doc_ids[0]
    pair_piece = lax.all_to_all(paired, "seq", split_axis=2, concat_axis=1, tiled=True)
    value_piece = lax.all_to_all(valued, "seq", split_axis=2, concat_axis=1, tiled=True)
    attended = attend_heads(
        pair_piece[0, :, 0], pair_piece[1, :, 0], value_piece[0, :, 0], documents
    )
    by_position = attended.reshape(seq_count, tokens, local_heads * HD)
    own_attended = lax.all_to_all(
        by_position, "seq", split_axis=0, concat_axis=2, tiled=True
    ).reshape(tokens, model_width)
    column_block = jnp.dot(
        lax.all_gather(own_attended, "dp", axis=0, tiled=True),
        out_weight,
        preferred_element_type=jnp.float32,
    ).astype(jnp.bfloat16)
    projected = lax.all_to_all(column_block, "dp", split_axis=0, concat_axis=1, tiled=True)
    residual = (resid[0].astype(jnp.float32) + projected.astype(jnp.float32)).astype(jnp.bfloat16)
    stream = residual.astype(jnp.float32)
    normed = (
        stream * lax.rsqrt(jnp.mean(stream * stream, axis=-1, keepdims=True) + norm_eps) * norm_gain
    ).astype(jnp.bfloat16)
    if expert_gate.shape[0] % SPLIT == 0:
        return gathered_layer(
            residual,
            normed,
            expert_ids,
            gate_vals,
            expert_gate,
            expert_up,
            expert_down,
            (shared_gate, shared_up, shared_down),
            shared_score,
        )
    shared_parts = shared_block(
        lax.all_gather(normed, "dp", axis=0, tiled=True), shared_gate, shared_up, shared_down
    )
    shared_sum = lax.psum_scatter(
        shared_parts.astype(jnp.bfloat16), "dp", scatter_dimension=0, tiled=True
    ).astype(jnp.float32)
    share_weight = jax.nn.sigmoid(jnp.dot(normed, shared_score, preferred_element_type=jnp.float32))
    routes = expert_ids[0]
    route_gates = gate_vals[0]
    slot_ids = slot_numbers(routes)
    slot_range = jnp.arange(EXPERTS * CAP, dtype=jnp.int32)
    picked = jnp.sum(
        (slot_ids[None, :, :] == slot_range[:, None, None]).astype(jnp.int32), axis=-1
    ).astype(jnp.bfloat16)
    buffer = jnp.dot(picked, normed, preferred_element_type=jnp.float32).astype(jnp.bfloat16)
    outgoing = jnp.broadcast_to(
        buffer.reshape(EXPERTS, 1, CAP, model_width), (EXPERTS, SPLIT, CAP, model_width)
    )
    own_pieces = expert_gate.shape[0]
    devices = seq_count * batch_count
    incoming = lax.all_to_all(
        outgoing.reshape(EXPERTS * SPLIT, CAP, model_width),
        ("seq", "dp"),
        split_axis=0,
        concat_axis=0,
        tiled=True,
    )
    results = piece_block(
        incoming.reshape(devices, own_pieces, CAP, model_width), expert_gate, expert_up, expert_down
    )
    returned = lax.all_to_all(
        results.reshape(devices * own_pieces, CAP, model_width),
        ("seq", "dp"),
        split_axis=0,
        concat_axis=0,
        tiled=True,
    )
    expert_out = jnp.sum(
        returned.reshape(EXPERTS, SPLIT, CAP, model_width).astype(jnp.float32), axis=1
    ).reshape(EXPERTS * CAP, model_width)
    fetched = jnp.take(expert_out, slot_ids.reshape(-1), axis=0).reshape(tokens, TOPK, model_width)
    routed = jnp.sum(route_gates[..., None] * fetched, axis=1)
    layer_out = residual.astype(jnp.float32) + routed + share_weight[:, None] * shared_sum
    return layer_out.astype(jnp.bfloat16)[None]


def solution(mesh):
    placed = (
        P(("groups", "dp"), "seq", None),
        P(None, ("groups", "dp"), "seq", None),
        P(("groups", "dp"), "seq", None),
        P(("groups", "dp"), None),
        P(None, "dp"),
        P(),
        P(("groups", "dp"), "seq", None),
        P(("groups", "dp"), "seq", None),
        P(("seq", "dp"), None, None),
        P(("seq", "dp"), None, None),
        P(("seq", "dp"), None, None),
        P(None, "dp"),
        P(None, "dp"),
        P("dp", None),
        P(),
    )
    return jax.shard_map(
        body,
        mesh=mesh,
        in_specs=placed,
        out_specs=P(("groups", "dp"), "seq", None),
        check_vma=False,
    )
```

```python
import functools
import math

import jax
import jax.numpy as jnp
from jax import lax
from jax.experimental import pallas as pl
from jax.experimental.pallas import tpu as pltpu
from jax.sharding import PartitionSpec as P

HD = 128
EXPERTS = 32
TOPK = 4
SPLIT = 4
CAP = 10


norm_eps = 1e-06


def slot_numbers(routes):
    flat_routes = routes.reshape(routes.shape[:-2] + (-1,))
    matches = (flat_routes[..., None] == jnp.arange(EXPERTS, dtype=jnp.int32)).astype(jnp.int32)
    ranked = jnp.sum(matches * (jnp.cumsum(matches, axis=-2) - 1), axis=-1)
    return (flat_routes * CAP + ranked).reshape(routes.shape)


def attend_heads(queries, key_rows, value_rows, documents):
    score_scale = 1.0 / math.sqrt(queries.shape[-1])
    scores = (
        jnp.einsum("qhd,khd->hqk", queries, key_rows, preferred_element_type=jnp.float32)
        * score_scale
    )
    positions = jnp.arange(queries.shape[0], dtype=jnp.int32)
    allowed = (positions[:, None] >= positions[None, :]) & (
        documents[:, None] == documents[None, :]
    )
    scores = jnp.where(allowed[None], scores, -1e30)
    row_max = jnp.max(scores, axis=-1, keepdims=True)
    lifted = jnp.exp(scores - row_max)
    weights = (lifted / jnp.sum(lifted, axis=-1, keepdims=True)).astype(jnp.bfloat16)
    return jnp.einsum(
        "hqk,khd->qhd", weights, value_rows, preferred_element_type=jnp.float32
    ).astype(jnp.bfloat16)


def piece_block(row_block, gate_matrix, up_matrix, down_matrix):
    gate_act = jnp.einsum(
        "npcd,pdf->npcf", row_block, gate_matrix, preferred_element_type=jnp.float32
    )
    up_act = jnp.einsum("npcd,pdf->npcf", row_block, up_matrix, preferred_element_type=jnp.float32)
    hidden = (jax.nn.silu(gate_act) * up_act).astype(jnp.bfloat16)
    return jnp.einsum(
        "npcf,pfd->npcd", hidden, down_matrix, preferred_element_type=jnp.float32
    ).astype(jnp.bfloat16)


def shared_block(row_block, gate_matrix, up_matrix, down_matrix):
    gate_act = jnp.dot(row_block, gate_matrix, preferred_element_type=jnp.float32)
    up_act = jnp.dot(row_block, up_matrix, preferred_element_type=jnp.float32)
    hidden = (jax.nn.silu(gate_act) * up_act).astype(jnp.bfloat16)
    return jnp.dot(hidden, down_matrix, preferred_element_type=jnp.float32)


MESH = pl.DeviceIdType.MESH


def remote(src, dst, send_sem, recv_sem, **where):
    return pltpu.make_async_remote_copy(
        src_ref=src,
        dst_ref=dst,
        send_sem=send_sem,
        recv_sem=recv_sem,
        device_id=where,
        device_id_type=MESH,
    )


def greet(peers):
    barrier = pltpu.get_barrier_semaphore()

    def hello(where):
        pl.semaphore_signal(barrier, inc=1, device_id=where, device_id_type=MESH)

    for ok, where in peers:
        if ok is True:
            hello(where)
        else:
            pl.when(ok)(functools.partial(hello, where))

    always = sum(1 for ok, _ in peers if ok is True)
    some = [ok for ok, _ in peers if ok is not True]
    if not some:
        pl.semaphore_wait(barrier, always)
        return
    first, second = some

    @pl.when(first & second)
    def _():
        pl.semaphore_wait(barrier, always + 2)

    @pl.when(first != second)
    def _():
        pl.semaphore_wait(barrier, always + 1)


def neighbours(s, d, batch):
    return [
        (True, {"seq": flip(s, 1), "dp": d}),
        (True, {"seq": flip(s, 2), "dp": d}),
        (d > 0, {"seq": s, "dp": d - 1}),
        (d < batch - 1, {"seq": s, "dp": d + 1}),
    ]


def flip(s, bit):
    return s + bit - 2 * bit * ((s // bit) % 2)


def line_kernel(seqs, batch, x_ref, t_ref, o_ref, ot_ref, zs, zr, ts, tr, ls):
    s, d = lax.axis_index("seq"), lax.axis_index("dp")
    n = seqs * batch
    me = s * batch + d
    others = []
    for k in range(1, n):
        to = lax.rem(me + k, n)
        others.append((True, {"seq": to // batch, "dp": lax.rem(to, batch)}))
    greet(others)
    own = pltpu.make_async_copy(x_ref, o_ref.at[d], ls.at[0])
    own_t = pltpu.make_async_copy(t_ref, ot_ref.at[me], ls.at[1])
    own.start()
    own_t.start()

    def step(way, k, block, src):
        return remote(
            src, o_ref.at[block], zs.at[way, k], zr.at[way, k], seq=s, dp=d + 1 - 2 * way
        )

    def sends(way, k):
        held = d >= k if way == 0 else d + k < batch
        return held & (d < batch - 1 if way == 0 else d > 0)

    def gets(way, k):
        return d - 1 - k >= 0 if way == 0 else d + 1 + k < batch

    for k in range(batch):
        for way in range(2):
            if k > 0:

                @pl.when(gets(way, k - 1))
                def _():
                    step(way, k - 1, d, x_ref).wait_recv()

            if k < batch - 1:

                @pl.when(sends(way, k))
                def _():
                    block = d - k + 2 * k * way
                    step(way, k, block, x_ref if k == 0 else o_ref.at[block]).start()

        if k == 0:
            for j, (_, where) in enumerate(others):
                remote(t_ref, ot_ref.at[me], ts.at[j], tr.at[j], **where).start()
    for k in range(batch - 1):
        for way in range(2):

            @pl.when(sends(way, k))
            def _():
                step(way, k, d, x_ref).wait_send()

    for j, (_, where) in enumerate(others):
        copy = remote(t_ref, ot_ref.at[me], ts.at[j], tr.at[j], **where)
        copy.wait_send()
        copy.wait_recv()
    own.wait()
    own_t.wait()


def pool_kernel(seqs, batch, x_ref, o_ref, ws, wr, bs, br, ys, yr, ps, pr, hs, hr, ls):
    s, d = lax.axis_index("seq"), lax.axis_index("dp")
    far, near = flip(s, 2), flip(s, 1)
    half = x_ref.shape[0] // 2
    low, high = pl.ds(0, half), pl.ds(half, half)
    greet(neighbours(s, d, batch))

    def at(ss, dd):
        return o_ref.at[ss * batch + dd]

    def wide(way, k, block, src):
        return remote(src, at(s, block), ws.at[way, k], wr.at[way, k], seq=s, dp=d + 1 - 2 * way)

    def thin(way, k, block):
        part = at(far, block).at[high]
        return remote(part, part, bs.at[way, k], br.at[way, k], seq=s, dp=d + 1 - 2 * way)

    def across(block):
        part = at(s, block).at[low]
        return remote(part, part, ys.at[block], yr.at[block], seq=far, dp=d)

    def across_own():
        return remote(x_ref, at(s, d), ys.at[batch], yr.at[batch], seq=far, dp=d)

    def beside(block, src=None):
        to = at(s, block)
        return remote(to if src is None else src, to, ps.at[block], pr.at[block], seq=near, dp=d)

    def beside_far(block, top):
        part = at(far, block).at[high if top else low]
        return remote(part, part, hs.at[top, block], hr.at[top, block], seq=near, dp=d)

    def sends(way, k):
        held = d >= k if way == 0 else d + k < batch
        return held & (d < batch - 1 if way == 0 else d > 0)

    def gets(way, k):
        return d - 1 - k >= 0 if way == 0 else d + 1 + k < batch

    own = pltpu.make_async_copy(x_ref, at(s, d), ls.at[0])
    own.start()
    for way in range(2):

        @pl.when(sends(way, 0))
        def _():
            wide(way, 0, d, x_ref).start()

    across_own().start()
    beside(d, x_ref).start()
    for k in range(1, batch + 1):
        for way in range(2):
            sign = 2 * way - 1
            if k < batch:

                @pl.when(gets(way, k - 1))
                def _():
                    wide(way, k - 1, d, x_ref).wait_recv()

                if k < batch - 1:

                    @pl.when(sends(way, k))
                    def _():
                        wide(way, k, d + sign * k, at(s, d + sign * k)).start()

                @pl.when(gets(way, k - 1))
                def _():
                    across(d + sign * k).start()
                    beside(d + sign * k).start()

            if k > 1:

                @pl.when(gets(way, k - 2))
                def _():
                    thin(way, k - 2, d).wait_recv()

                if k < batch:

                    @pl.when(sends(way, k - 1))
                    def _():
                        thin(way, k - 1, d + sign * (k - 1)).start()

                @pl.when(gets(way, k - 2))
                def _():
                    beside_far(d + sign * (k - 1), 1).start()

        if k == 1:
            across_own().wait_recv()
            for way in range(2):

                @pl.when(sends(way, 0))
                def _():
                    thin(way, 0, d).start()

            beside_far(d, 0).start()
            beside_far(d, 1).start()
    for off in range(1, batch):
        block = lax.rem(d + off, batch)
        across(block).wait_recv()
        beside_far(block, 0).start()
    for block in range(batch):
        beside(block).wait_recv()
        beside_far(block, 0).wait_recv()
        beside_far(block, 1).wait_recv()
    for k in range(batch - 1):
        for way in range(2):

            @pl.when(sends(way, k))
            def _():
                wide(way, k, d, x_ref).wait_send()
                thin(way, k, d).wait_send()

    across_own().wait_send()
    for off in range(1, batch):
        across(lax.rem(d + off, batch)).wait_send()
    for block in range(batch):
        beside(block).wait_send()
        beside_far(block, 0).wait_send()
        beside_far(block, 1).wait_send()
    own.wait()


def scatter_kernel(
    seqs, batch, x_ref, o_ref, near_buf, acc, y_buf, yb_buf, z_buf, ds, dr, ys, yr, zs, zr
):
    s, d = lax.axis_index("seq"), lax.axis_index("dp")
    far, near, cross = flip(s, 2), flip(s, 1), flip(flip(s, 1), 2)
    half = x_ref.shape[1] // 2
    low, high = pl.ds(0, half), pl.ds(half, half)
    greet(neighbours(s, d, batch))

    def chip(which, block):
        row = (cross if which else near) * batch + block
        return remote(
            x_ref.at[row],
            near_buf.at[which, block],
            ds.at[which, block],
            dr.at[which, block],
            seq=near,
            dp=d,
        )

    def add(a, b):
        return (a.astype(jnp.float32) + b.astype(jnp.float32)).astype(jnp.bfloat16)

    def across(block):
        return remote(
            acc.at[1, block, low], y_buf.at[block], ys.at[block], yr.at[block], seq=far, dp=d
        )

    def across_last():
        return remote(
            acc.at[1, d, high], yb_buf, ys.at[batch], yr.at[batch], seq=far, dp=d
        )

    flows = ((1, high), (0, high), (0, low))

    def hop(flow, way, block):
        which, part = flows[flow]
        return remote(
            acc.at[which, block, part],
            z_buf.at[flow, way, block],
            zs.at[flow, block],
            zr.at[flow, way, block],
            seq=s,
            dp=d + 1 - 2 * way,
        )

    def merge(flow, way, block):
        which, part = flows[flow]
        hop(flow, way, block).wait_recv()
        acc[which, block, part] = add(acc[which, block, part], z_buf[flow, way, block])

    for which in (1, 0):
        for block in range(batch):
            chip(which, block).start()
    for which in (1, 0):
        for block in range(batch):
            chip(which, block).wait_recv()
            row = (far if which else s) * batch + block
            acc[which, block] = add(x_ref[row], near_buf[which, block])
            if which:
                across(block).start()

    def line(flow):
        for k in range(batch - 1):
            for way in range(2):
                block = k if way else batch - 1 - k
                inner = d < batch - 1 if way else d > 0

                @pl.when((d > block if way else d < block) & inner)
                def _():
                    merge(flow, way, block)

                @pl.when(d > block if way else d < block)
                def _():
                    hop(flow, way, block).start()

    def land(flow):
        for way in range(2):

            @pl.when(d < batch - 1 if way else d > 0)
            def _():
                merge(flow, way, d)

    line(0)
    line(1)
    for block in range(batch):
        across(block).wait_recv()
        acc[0, block, low] = add(acc[0, block, low], y_buf[block])
    line(2)
    land(0)
    across_last().start()
    land(1)
    land(2)
    across_last().wait_recv()
    acc[0, d, high] = add(acc[0, d, high], yb_buf[...])
    o_ref[...] = acc[0, d]
    for which in (1, 0):
        for block in range(batch):
            chip(which, block).wait_send()
    for block in range(batch):
        across(block).wait_send()
    across_last().wait_send()
    for flow in range(3):
        for block in range(batch):

            @pl.when(d < block)
            def _():
                hop(flow, 0, block).wait_send()

            @pl.when(d > block)
            def _():
                hop(flow, 1, block).wait_send()


VMEM = pl.BlockSpec(memory_space=pltpu.VMEM)
DMA = pltpu.SemaphoreType.DMA


def params(number):
    return pltpu.CompilerParams(
        collective_id=number, has_side_effects=True, vmem_limit_bytes=24 << 20
    )


def line_gather(x, table):
    seqs, batch = lax.axis_size("seq"), lax.axis_size("dp")
    n = seqs * batch
    return pl.pallas_call(
        functools.partial(line_kernel, seqs, batch),
        out_shape=(
            jax.ShapeDtypeStruct((batch,) + x.shape, x.dtype),
            jax.ShapeDtypeStruct((n,) + table.shape, table.dtype),
        ),
        in_specs=[VMEM, VMEM],
        out_specs=(VMEM, VMEM),
        scratch_shapes=[
            DMA((2, batch)),
            DMA((2, batch)),
            DMA((n,)),
            DMA((n,)),
            DMA((2,)),
        ],
        compiler_params=params(1),
    )(x, table)


def pool_gather(x):
    seqs, batch = lax.axis_size("seq"), lax.axis_size("dp")
    return pl.pallas_call(
        functools.partial(pool_kernel, seqs, batch),
        out_shape=jax.ShapeDtypeStruct((seqs * batch,) + x.shape, x.dtype),
        in_specs=[VMEM],
        out_specs=VMEM,
        scratch_shapes=[
            DMA((2, batch)),
            DMA((2, batch)),
            DMA((2, batch)),
            DMA((2, batch)),
            DMA((batch + 1,)),
            DMA((batch + 1,)),
            DMA((batch,)),
            DMA((batch,)),
            DMA((2, batch)),
            DMA((2, batch)),
            DMA((1,)),
        ],
        compiler_params=params(2),
    )(x)


def pool_scatter(x):
    seqs, batch = lax.axis_size("seq"), lax.axis_size("dp")
    tokens, width = x.shape[1:]
    half = tokens // 2
    return pl.pallas_call(
        functools.partial(scatter_kernel, seqs, batch),
        out_shape=jax.ShapeDtypeStruct((tokens, width), x.dtype),
        in_specs=[VMEM],
        out_specs=VMEM,
        scratch_shapes=[
            pltpu.VMEM((2, batch, tokens, width), x.dtype),
            pltpu.VMEM((2, batch, tokens, width), x.dtype),
            pltpu.VMEM((batch, half, width), x.dtype),
            pltpu.VMEM((half, width), x.dtype),
            pltpu.VMEM((3, 2, batch, half, width), x.dtype),
            DMA((2, batch)),
            DMA((2, batch)),
            DMA((batch + 1,)),
            DMA((batch + 1,)),
            DMA((3, batch)),
            DMA((3, 2, batch)),
        ],
        compiler_params=params(3),
    )(x)


def gathered_layer(residual, normed, table, gate, up, down, shared, score):
    seq_count, batch_count = lax.axis_size("seq"), lax.axis_size("dp")
    devices = seq_count * batch_count
    tokens, width = normed.shape
    own_experts = gate.shape[0] // SPLIT
    room = devices * CAP
    me = lax.axis_index("seq") * batch_count + lax.axis_index("dp")
    mine = (me * own_experts + jnp.arange(own_experts)).astype(jnp.float32)
    named = (table[:, :TOPK, None] == mine).astype(jnp.float32)
    weight = jnp.sum(named * table[:, TOPK:, None], axis=1)
    named = jnp.sum(named, axis=1)
    total = devices * tokens
    order = jnp.arange(total)
    before = (order[None, :] < order[:, None]).astype(jnp.bfloat16)
    rank = jnp.dot(before, named.astype(jnp.bfloat16), preferred_element_type=jnp.float32)
    spot = jnp.where(named > 0, rank, -1.0)
    pick = spot.T[:, None, :] == jnp.arange(room, dtype=jnp.float32)[None, :, None]
    slot_gate = jnp.sum(jnp.where(pick, weight.T[:, None, :], 0.0), axis=-1)
    pick = pick.astype(jnp.bfloat16).reshape(own_experts * room, total)

    pool = pool_gather(normed).reshape(total, width)
    rows = jnp.dot(pick, pool, preferred_element_type=jnp.float32).astype(jnp.bfloat16)
    rows = rows.reshape(own_experts, room, width)
    gate = gate.reshape((own_experts, SPLIT) + gate.shape[1:])
    up = up.reshape((own_experts, SPLIT) + up.shape[1:])
    down = down.reshape((own_experts, SPLIT) + down.shape[1:])
    gate_act = jnp.einsum("ecd,ebdf->ebcf", rows, gate, preferred_element_type=jnp.float32)
    up_act = jnp.einsum("ecd,ebdf->ebcf", rows, up, preferred_element_type=jnp.float32)
    hidden = (jax.nn.silu(gate_act) * up_act).astype(jnp.bfloat16)
    expert_out = jnp.einsum("ebcf,ebfd->ecd", hidden, down, preferred_element_type=jnp.float32)
    expert_out = (expert_out * slot_gate[..., None]).astype(jnp.bfloat16)
    partial = lax.dot_general(
        pick,
        expert_out.reshape(own_experts * room, width),
        (((0,), (0,)), ((), ())),
        preferred_element_type=jnp.float32,
    ).reshape(seq_count, batch_count * tokens, width)
    s = lax.axis_index("seq")
    line = lax.dynamic_slice_in_dim(pool, s * batch_count * tokens, batch_count * tokens)
    share_weight = jax.nn.sigmoid(jnp.dot(line, score, preferred_element_type=jnp.float32))
    shared_part = shared_block(line, *shared) * share_weight[:, None]
    here = (jnp.arange(seq_count) == s)[:, None, None]
    partial = jnp.where(here, partial + shared_part[None], partial).astype(jnp.bfloat16)
    summed = pool_scatter(partial.reshape(devices, tokens, width))
    out = residual.astype(jnp.float32) + summed.astype(jnp.float32)
    return out.astype(jnp.bfloat16)[None]


def body(
    resid,
    queries_keys,
    values,
    doc_ids,
    out_weight,
    norm_gain,
    expert_ids,
    gate_vals,
    expert_gate,
    expert_up,
    expert_down,
    shared_gate,
    shared_up,
    shared_down,
    shared_score,
):
    seq_count = lax.axis_size("seq")
    batch_count = lax.axis_size("dp")
    tokens = resid.shape[1]
    model_width = resid.shape[2]
    local_heads = model_width // HD // seq_count
    paired = queries_keys.reshape(2, tokens, seq_count, local_heads, HD)
    valued = values.reshape(1, tokens, seq_count, local_heads, HD)
    documents = doc_ids[0]
    pair_piece = lax.all_to_all(paired, "seq", split_axis=2, concat_axis=1, tiled=True)
    value_piece = lax.all_to_all(valued, "seq", split_axis=2, concat_axis=1, tiled=True)
    attended = attend_heads(
        pair_piece[0, :, 0], pair_piece[1, :, 0], value_piece[0, :, 0], documents
    )
    by_position = attended.reshape(seq_count, tokens, local_heads * HD)
    own_attended = lax.all_to_all(
        by_position, "seq", split_axis=0, concat_axis=2, tiled=True
    ).reshape(tokens, model_width)
    dense = expert_gate.shape[0] % SPLIT == 0 and seq_count == 4 and batch_count > 1 and tokens % 32 == 0
    if dense:
        table = jnp.concatenate([expert_ids[0].astype(jnp.float32), gate_vals[0]], axis=1)
        table = jnp.pad(table.T, ((0, 0), (0, -tokens % 128)))
        gathered, table = line_gather(own_attended, table)
        gathered = gathered.reshape(batch_count * tokens, model_width)
        table = table[:, :, :tokens].swapaxes(1, 2).reshape(-1, 2 * TOPK)
    else:
        gathered = lax.all_gather(own_attended, "dp", axis=0, tiled=True)
    column_block = jnp.dot(
        gathered,
        out_weight,
        preferred_element_type=jnp.float32,
    ).astype(jnp.bfloat16)
    projected = lax.all_to_all(column_block, "dp", split_axis=0, concat_axis=1, tiled=True)
    residual = (resid[0].astype(jnp.float32) + projected.astype(jnp.float32)).astype(jnp.bfloat16)
    stream = residual.astype(jnp.float32)
    normed = (
        stream * lax.rsqrt(jnp.mean(stream * stream, axis=-1, keepdims=True) + norm_eps) * norm_gain
    ).astype(jnp.bfloat16)
    if dense:
        return gathered_layer(
            residual,
            normed,
            table,
            expert_gate,
            expert_up,
            expert_down,
            (shared_gate, shared_up, shared_down),
            shared_score,
        )
    shared_parts = shared_block(
        lax.all_gather(normed, "dp", axis=0, tiled=True), shared_gate, shared_up, shared_down
    )
    shared_sum = lax.psum_scatter(
        shared_parts.astype(jnp.bfloat16), "dp", scatter_dimension=0, tiled=True
    ).astype(jnp.float32)
    share_weight = jax.nn.sigmoid(jnp.dot(normed, shared_score, preferred_element_type=jnp.float32))
    routes = expert_ids[0]
    route_gates = gate_vals[0]
    slot_ids = slot_numbers(routes)
    slot_range = jnp.arange(EXPERTS * CAP, dtype=jnp.int32)
    picked = jnp.sum(
        (slot_ids[None, :, :] == slot_range[:, None, None]).astype(jnp.int32), axis=-1
    ).astype(jnp.bfloat16)
    buffer = jnp.dot(picked, normed, preferred_element_type=jnp.float32).astype(jnp.bfloat16)
    outgoing = jnp.broadcast_to(
        buffer.reshape(EXPERTS, 1, CAP, model_width), (EXPERTS, SPLIT, CAP, model_width)
    )
    own_pieces = expert_gate.shape[0]
    devices = seq_count * batch_count
    incoming = lax.all_to_all(
        outgoing.reshape(EXPERTS * SPLIT, CAP, model_width),
        ("seq", "dp"),
        split_axis=0,
        concat_axis=0,
        tiled=True,
    )
    results = piece_block(
        incoming.reshape(devices, own_pieces, CAP, model_width), expert_gate, expert_up, expert_down
    )
    returned = lax.all_to_all(
        results.reshape(devices * own_pieces, CAP, model_width),
        ("seq", "dp"),
        split_axis=0,
        concat_axis=0,
        tiled=True,
    )
    expert_out = jnp.sum(
        returned.reshape(EXPERTS, SPLIT, CAP, model_width).astype(jnp.float32), axis=1
    ).reshape(EXPERTS * CAP, model_width)
    fetched = jnp.take(expert_out, slot_ids.reshape(-1), axis=0).reshape(tokens, TOPK, model_width)
    routed = jnp.sum(route_gates[..., None] * fetched, axis=1)
    layer_out = residual.astype(jnp.float32) + routed + share_weight[:, None] * shared_sum
    return layer_out.astype(jnp.bfloat16)[None]


def solution(mesh):
    placed = (
        P(("groups", "dp"), "seq", None),
        P(None, ("groups", "dp"), "seq", None),
        P(("groups", "dp"), "seq", None),
        P(("groups", "dp"), None),
        P(None, "dp"),
        P(),
        P(("groups", "dp"), "seq", None),
        P(("groups", "dp"), "seq", None),
        P(("seq", "dp"), None, None),
        P(("seq", "dp"), None, None),
        P(("seq", "dp"), None, None),
        P(None, "dp"),
        P(None, "dp"),
        P("dp", None),
        P(),
    )
    return jax.shard_map(
        body,
        mesh=mesh,
        in_specs=placed,
        out_specs=P(("groups", "dp"), "seq", None),
        check_vma=False,
    )
```

```python
import functools
import math

import jax
import jax.numpy as jnp
from jax import lax
from jax.experimental import pallas as pl
from jax.experimental.pallas import tpu as pltpu
from jax.sharding import PartitionSpec as P

HD = 128
EXPERTS = 32
TOPK = 4
SPLIT = 4
CAP = 10


norm_eps = 1e-06


def slot_numbers(routes):
    flat_routes = routes.reshape(routes.shape[:-2] + (-1,))
    matches = (flat_routes[..., None] == jnp.arange(EXPERTS, dtype=jnp.int32)).astype(jnp.int32)
    ranked = jnp.sum(matches * (jnp.cumsum(matches, axis=-2) - 1), axis=-1)
    return (flat_routes * CAP + ranked).reshape(routes.shape)


def attend_heads(queries, key_rows, value_rows, documents):
    score_scale = 1.0 / math.sqrt(queries.shape[-1])
    scores = (
        jnp.einsum("qhd,khd->hqk", queries, key_rows, preferred_element_type=jnp.float32)
        * score_scale
    )
    positions = jnp.arange(queries.shape[0], dtype=jnp.int32)
    allowed = (positions[:, None] >= positions[None, :]) & (
        documents[:, None] == documents[None, :]
    )
    scores = jnp.where(allowed[None], scores, -1e30)
    row_max = jnp.max(scores, axis=-1, keepdims=True)
    lifted = jnp.exp(scores - row_max)
    weights = (lifted / jnp.sum(lifted, axis=-1, keepdims=True)).astype(jnp.bfloat16)
    return jnp.einsum(
        "hqk,khd->qhd", weights, value_rows, preferred_element_type=jnp.float32
    ).astype(jnp.bfloat16)


def piece_block(row_block, gate_matrix, up_matrix, down_matrix):
    gate_act = jnp.einsum(
        "npcd,pdf->npcf", row_block, gate_matrix, preferred_element_type=jnp.float32
    )
    up_act = jnp.einsum("npcd,pdf->npcf", row_block, up_matrix, preferred_element_type=jnp.float32)
    hidden = (jax.nn.silu(gate_act) * up_act).astype(jnp.bfloat16)
    return jnp.einsum(
        "npcf,pfd->npcd", hidden, down_matrix, preferred_element_type=jnp.float32
    ).astype(jnp.bfloat16)


def shared_block(row_block, gate_matrix, up_matrix, down_matrix):
    gate_act = jnp.dot(row_block, gate_matrix, preferred_element_type=jnp.float32)
    up_act = jnp.dot(row_block, up_matrix, preferred_element_type=jnp.float32)
    hidden = (jax.nn.silu(gate_act) * up_act).astype(jnp.bfloat16)
    return jnp.dot(hidden, down_matrix, preferred_element_type=jnp.float32)


MESH = pl.DeviceIdType.MESH


def remote(src, dst, send_sem, recv_sem, **where):
    return pltpu.make_async_remote_copy(
        src_ref=src,
        dst_ref=dst,
        send_sem=send_sem,
        recv_sem=recv_sem,
        device_id=where,
        device_id_type=MESH,
    )


def greet(peers):
    barrier = pltpu.get_barrier_semaphore()

    def hello(where):
        pl.semaphore_signal(barrier, inc=1, device_id=where, device_id_type=MESH)

    for ok, where in peers:
        if ok is True:
            hello(where)
        else:
            pl.when(ok)(functools.partial(hello, where))

    always = sum(1 for ok, _ in peers if ok is True)
    some = [ok for ok, _ in peers if ok is not True]
    if not some:
        pl.semaphore_wait(barrier, always)
        return
    first, second = some

    @pl.when(first & second)
    def _():
        pl.semaphore_wait(barrier, always + 2)

    @pl.when(first != second)
    def _():
        pl.semaphore_wait(barrier, always + 1)


def neighbours(s, d, batch):
    return [
        (True, {"seq": flip(s, 1), "dp": d}),
        (True, {"seq": flip(s, 2), "dp": d}),
        (d > 0, {"seq": s, "dp": d - 1}),
        (d < batch - 1, {"seq": s, "dp": d + 1}),
    ]


def flip(s, bit):
    return s + bit - 2 * bit * ((s // bit) % 2)


def line_kernel(
    seqs, batch, q_ref, v_ref, row_ref, col_ref, t_ref, o_ref, ot_ref,
    got, att, zs, zr, ts, tr, ls, qs, qr, ats, atr,
):
    s, d = lax.axis_index("seq"), lax.axis_index("dp")
    n = seqs * batch
    me = s * batch + d
    tokens, width = v_ref.shape
    part = width // seqs
    others = []
    for k in range(1, n):
        to = lax.rem(me + k, n)
        others.append((True, {"seq": to // batch, "dp": lax.rem(to, batch)}))
    greet(others)

    def columns(who):
        return pl.ds(pl.multiple_of(who * part, 128), part)

    def rows(who):
        return pl.ds(pl.multiple_of(who * tokens, 16), tokens)

    def source(which):
        return v_ref if which == 2 else q_ref.at[which]

    def deal(which, k):
        to = lax.rem(s + k, seqs)
        return remote(
            source(which).at[:, columns(to)],
            got.at[which, rows(s)],
            qs.at[which, k],
            qr.at[which, k],
            seq=to,
            dp=d,
        )

    def keep(which):
        return pltpu.make_async_copy(
            source(which).at[:, columns(s)], got.at[which, rows(s)], ls.at[which]
        )

    def back(k):
        to = lax.rem(s + k, seqs)
        return remote(
            att.at[rows(to)], o_ref.at[d, :, columns(s)], ats.at[k], atr.at[k], seq=to, dp=d
        )

    for which in range(3):
        for k in range(1, seqs):
            deal(which, k).start()
        keep(which).start()
    own_t = pltpu.make_async_copy(t_ref, ot_ref.at[me], ls.at[3])
    own_t.start()
    for which in range(3):
        for k in range(1, seqs):
            deal(which, k).wait_recv()
        keep(which).wait()
    length = tokens * seqs
    seen = (
        lax.broadcasted_iota(jnp.int32, (length, length), 0)
        >= lax.broadcasted_iota(jnp.int32, (length, length), 1)
    ) & (col_ref[...] == row_ref[...])
    for h in range(part // HD):
        at = pl.ds(h * HD, HD)
        scores = lax.dot_general(
            got[0, :, at], got[1, :, at], (((1,), (1,)), ((), ())),
            preferred_element_type=jnp.float32,
        )
        scores = jnp.where(seen, scores * (1.0 / math.sqrt(HD)), -1e30)
        lifted = jnp.exp(scores - jnp.max(scores, axis=-1, keepdims=True))
        probs = (lifted / jnp.sum(lifted, axis=-1, keepdims=True)).astype(jnp.bfloat16)
        att[:, at] = jnp.dot(
            probs, got[2, :, at], preferred_element_type=jnp.float32
        ).astype(jnp.bfloat16)
    for k in range(1, seqs):
        back(k).start()
    own = pltpu.make_async_copy(att.at[rows(s)], o_ref.at[d, :, columns(s)], ls.at[4])
    own.start()
    for k in range(1, seqs):
        back(k).wait_recv()
    own.wait()
    x_ref = o_ref.at[d]

    def step(way, k, block, src):
        return remote(
            src, o_ref.at[block], zs.at[way, k], zr.at[way, k], seq=s, dp=d + 1 - 2 * way
        )

    def sends(way, k):
        held = d >= k if way == 0 else d + k < batch
        return held & (d < batch - 1 if way == 0 else d > 0)

    def gets(way, k):
        return d - 1 - k >= 0 if way == 0 else d + 1 + k < batch

    for k in range(batch):
        for way in range(2):
            if k > 0:

                @pl.when(gets(way, k - 1))
                def _():
                    step(way, k - 1, d, x_ref).wait_recv()

            if k < batch - 1:

                @pl.when(sends(way, k))
                def _():
                    block = d - k + 2 * k * way
                    step(way, k, block, x_ref if k == 0 else o_ref.at[block]).start()

        if k == 0:
            for j, (_, where) in enumerate(others):
                remote(t_ref, ot_ref.at[me], ts.at[j], tr.at[j], **where).start()
    for k in range(batch - 1):
        for way in range(2):

            @pl.when(sends(way, k))
            def _():
                step(way, k, d, x_ref).wait_send()

    for j, (_, where) in enumerate(others):
        copy = remote(t_ref, ot_ref.at[me], ts.at[j], tr.at[j], **where)
        copy.wait_send()
        copy.wait_recv()
    own_t.wait()
    for k in range(1, seqs):
        back(k).wait_send()
        for which in range(3):
            deal(which, k).wait_send()


def pool_kernel(
    seqs, batch, g_ref, w_ref, r_ref, gain_ref, o_ref, res_ref, x_ref, cb, pb, cs, cr, ws, wr, bs, br, ys, yr, ps, pr, hs, hr, ls
):
    s, d = lax.axis_index("seq"), lax.axis_index("dp")
    far, near = flip(s, 2), flip(s, 1)
    half = x_ref.shape[0] // 2
    low, high = pl.ds(0, half), pl.ds(half, half)
    mates = [(True, {"seq": near, "dp": d}), (True, {"seq": far, "dp": d})]
    for k in range(1, batch):
        mates.append((True, {"seq": s, "dp": lax.rem(d + k, batch)}))
    greet(mates)

    def hand(k):
        to = lax.rem(d + k, batch)
        return remote(cb.at[to], pb.at[d], cs.at[k], cr.at[k], seq=s, dp=to)

    tokens, width = x_ref.shape
    part = width // batch
    block = jnp.dot(
        g_ref[...].reshape(batch * tokens, width), w_ref[...], preferred_element_type=jnp.float32
    )
    cb[...] = block.astype(jnp.bfloat16).reshape(batch, tokens, part)
    for k in range(1, batch):
        hand(k).start()
    mine = pltpu.make_async_copy(cb.at[d], pb.at[d], ls.at[1])
    mine.start()
    for k in range(1, batch):
        hand(k).wait_recv()
    mine.wait()
    squares = jnp.zeros((tokens, 1), jnp.float32)
    for p in range(batch):
        at = pl.ds(p * part, part)
        stream = (r_ref[:, at].astype(jnp.float32) + pb[p].astype(jnp.float32)).astype(jnp.bfloat16)
        res_ref[:, at] = stream
        stream = stream.astype(jnp.float32)
        squares += jnp.sum(stream * stream, axis=-1, keepdims=True)
    scale = lax.rsqrt(squares / width + norm_eps)
    x_ref[...] = (res_ref[...].astype(jnp.float32) * scale * gain_ref[...]).astype(jnp.bfloat16)

    def at(ss, dd):
        return o_ref.at[ss * batch + dd]

    def wide(way, k, block, src):
        return remote(src, at(s, block), ws.at[way, k], wr.at[way, k], seq=s, dp=d + 1 - 2 * way)

    def thin(way, k, block):
        part = at(far, block).at[high]
        return remote(part, part, bs.at[way, k], br.at[way, k], seq=s, dp=d + 1 - 2 * way)

    def across(block):
        part = at(s, block).at[low]
        return remote(part, part, ys.at[block], yr.at[block], seq=far, dp=d)

    def across_own():
        return remote(x_ref, at(s, d), ys.at[batch], yr.at[batch], seq=far, dp=d)

    def beside(block, src=None):
        to = at(s, block)
        return remote(to if src is None else src, to, ps.at[block], pr.at[block], seq=near, dp=d)

    def beside_far(block, top):
        part = at(far, block).at[high if top else low]
        return remote(part, part, hs.at[top, block], hr.at[top, block], seq=near, dp=d)

    def sends(way, k):
        held = d >= k if way == 0 else d + k < batch
        return held & (d < batch - 1 if way == 0 else d > 0)

    def gets(way, k):
        return d - 1 - k >= 0 if way == 0 else d + 1 + k < batch

    own = pltpu.make_async_copy(x_ref, at(s, d), ls.at[0])
    own.start()
    for way in range(2):

        @pl.when(sends(way, 0))
        def _():
            wide(way, 0, d, x_ref).start()

    across_own().start()
    beside(d, x_ref).start()
    for k in range(1, batch + 1):
        for way in range(2):
            sign = 2 * way - 1
            if k < batch:

                @pl.when(gets(way, k - 1))
                def _():
                    wide(way, k - 1, d, x_ref).wait_recv()

                if k < batch - 1:

                    @pl.when(sends(way, k))
                    def _():
                        wide(way, k, d + sign * k, at(s, d + sign * k)).start()

                @pl.when(gets(way, k - 1))
                def _():
                    across(d + sign * k).start()
                    beside(d + sign * k).start()

            if k > 1:

                @pl.when(gets(way, k - 2))
                def _():
                    thin(way, k - 2, d).wait_recv()

                if k < batch:

                    @pl.when(sends(way, k - 1))
                    def _():
                        thin(way, k - 1, d + sign * (k - 1)).start()

                @pl.when(gets(way, k - 2))
                def _():
                    beside_far(d + sign * (k - 1), 1).start()

        if k == 1:
            across_own().wait_recv()
            for way in range(2):

                @pl.when(sends(way, 0))
                def _():
                    thin(way, 0, d).start()

            beside_far(d, 0).start()
            beside_far(d, 1).start()
    for off in range(1, batch):
        block = lax.rem(d + off, batch)
        across(block).wait_recv()
        beside_far(block, 0).start()
    for block in range(batch):
        beside(block).wait_recv()
        beside_far(block, 0).wait_recv()
        beside_far(block, 1).wait_recv()
    for k in range(batch - 1):
        for way in range(2):

            @pl.when(sends(way, k))
            def _():
                wide(way, k, d, x_ref).wait_send()
                thin(way, k, d).wait_send()

    across_own().wait_send()
    for off in range(1, batch):
        across(lax.rem(d + off, batch)).wait_send()
    for block in range(batch):
        beside(block).wait_send()
        beside_far(block, 0).wait_send()
        beside_far(block, 1).wait_send()
    own.wait()
    for k in range(1, batch):
        hand(k).wait_send()


def scatter_kernel(
    seqs, batch, x_ref, o_ref, near_buf, acc, y_buf, yb_buf, z_buf, ds, dr, ys, yr, zs, zr
):
    s, d = lax.axis_index("seq"), lax.axis_index("dp")
    far, near, cross = flip(s, 2), flip(s, 1), flip(flip(s, 1), 2)
    half = x_ref.shape[1] // 2
    low, high = pl.ds(0, half), pl.ds(half, half)
    greet(neighbours(s, d, batch))

    def chip(which, block):
        row = (cross if which else near) * batch + block
        return remote(
            x_ref.at[row],
            near_buf.at[which, block],
            ds.at[which, block],
            dr.at[which, block],
            seq=near,
            dp=d,
        )

    def add(a, b):
        return (a.astype(jnp.float32) + b.astype(jnp.float32)).astype(jnp.bfloat16)

    def across(block):
        return remote(
            acc.at[1, block, low], y_buf.at[block], ys.at[block], yr.at[block], seq=far, dp=d
        )

    def across_last():
        return remote(
            acc.at[1, d, high], yb_buf, ys.at[batch], yr.at[batch], seq=far, dp=d
        )

    flows = ((1, high), (0, high), (0, low))

    def hop(flow, way, block):
        which, part = flows[flow]
        return remote(
            acc.at[which, block, part],
            z_buf.at[flow, way, block],
            zs.at[flow, block],
            zr.at[flow, way, block],
            seq=s,
            dp=d + 1 - 2 * way,
        )

    def merge(flow, way, block):
        which, part = flows[flow]
        hop(flow, way, block).wait_recv()
        acc[which, block, part] = add(acc[which, block, part], z_buf[flow, way, block])

    for which in (1, 0):
        for block in range(batch):
            chip(which, block).start()
    for which in (1, 0):
        for block in range(batch):
            chip(which, block).wait_recv()
            row = (far if which else s) * batch + block
            acc[which, block] = add(x_ref[row], near_buf[which, block])
            if which:
                across(block).start()

    def line(flow):
        for k in range(batch - 1):
            for way in range(2):
                block = k if way else batch - 1 - k
                inner = d < batch - 1 if way else d > 0

                @pl.when((d > block if way else d < block) & inner)
                def _():
                    merge(flow, way, block)

                @pl.when(d > block if way else d < block)
                def _():
                    hop(flow, way, block).start()

    def land(flow):
        for way in range(2):

            @pl.when(d < batch - 1 if way else d > 0)
            def _():
                merge(flow, way, d)

    line(0)
    line(1)
    for block in range(batch):
        across(block).wait_recv()
        acc[0, block, low] = add(acc[0, block, low], y_buf[block])
    line(2)
    land(0)
    across_last().start()
    land(1)
    land(2)
    across_last().wait_recv()
    acc[0, d, high] = add(acc[0, d, high], yb_buf[...])
    o_ref[...] = acc[0, d]
    for which in (1, 0):
        for block in range(batch):
            chip(which, block).wait_send()
    for block in range(batch):
        across(block).wait_send()
    across_last().wait_send()
    for flow in range(3):
        for block in range(batch):

            @pl.when(d < block)
            def _():
                hop(flow, 0, block).wait_send()

            @pl.when(d > block)
            def _():
                hop(flow, 1, block).wait_send()


VMEM = pl.BlockSpec(memory_space=pltpu.VMEM)
DMA = pltpu.SemaphoreType.DMA


def params(number):
    return pltpu.CompilerParams(
        collective_id=number, has_side_effects=True, vmem_limit_bytes=24 << 20
    )


def attend_gather(queries_keys, values, documents, table):
    seqs, batch = lax.axis_size("seq"), lax.axis_size("dp")
    n = seqs * batch
    tokens, width = values.shape
    return pl.pallas_call(
        functools.partial(line_kernel, seqs, batch),
        out_shape=(
            jax.ShapeDtypeStruct((batch, tokens, width), values.dtype),
            jax.ShapeDtypeStruct((n,) + table.shape, table.dtype),
        ),
        in_specs=[VMEM] * 5,
        out_specs=(VMEM, VMEM),
        scratch_shapes=[
            pltpu.VMEM((3, seqs * tokens, width // seqs), values.dtype),
            pltpu.VMEM((seqs * tokens, width // seqs), values.dtype),
            DMA((2, batch)),
            DMA((2, batch)),
            DMA((n,)),
            DMA((n,)),
            DMA((5,)),
            DMA((3, seqs)),
            DMA((3, seqs)),
            DMA((seqs,)),
            DMA((seqs,)),
        ],
        compiler_params=params(1),
    )(queries_keys, values, documents[None, :], documents[:, None], table)


def pool_gather(gathered, weight, resid, gain):
    seqs, batch = lax.axis_size("seq"), lax.axis_size("dp")
    tokens, width = resid.shape
    return pl.pallas_call(
        functools.partial(pool_kernel, seqs, batch),
        out_shape=(
            jax.ShapeDtypeStruct((seqs * batch,) + resid.shape, resid.dtype),
            jax.ShapeDtypeStruct(resid.shape, resid.dtype),
        ),
        in_specs=[VMEM] * 4,
        out_specs=(VMEM, VMEM),
        scratch_shapes=[
            pltpu.VMEM(resid.shape, resid.dtype),
            pltpu.VMEM((batch, tokens, width // batch), resid.dtype),
            pltpu.VMEM((batch, tokens, width // batch), resid.dtype),
            DMA((batch,)),
            DMA((batch,)),
            DMA((2, batch)),
            DMA((2, batch)),
            DMA((2, batch)),
            DMA((2, batch)),
            DMA((batch + 1,)),
            DMA((batch + 1,)),
            DMA((batch,)),
            DMA((batch,)),
            DMA((2, batch)),
            DMA((2, batch)),
            DMA((2,)),
        ],
        compiler_params=params(2),
    )(gathered, weight, resid, gain[None, :])


def pool_scatter(x):
    seqs, batch = lax.axis_size("seq"), lax.axis_size("dp")
    tokens, width = x.shape[1:]
    half = tokens // 2
    return pl.pallas_call(
        functools.partial(scatter_kernel, seqs, batch),
        out_shape=jax.ShapeDtypeStruct((tokens, width), x.dtype),
        in_specs=[VMEM],
        out_specs=VMEM,
        scratch_shapes=[
            pltpu.VMEM((2, batch, tokens, width), x.dtype),
            pltpu.VMEM((2, batch, tokens, width), x.dtype),
            pltpu.VMEM((batch, half, width), x.dtype),
            pltpu.VMEM((half, width), x.dtype),
            pltpu.VMEM((3, 2, batch, half, width), x.dtype),
            DMA((2, batch)),
            DMA((2, batch)),
            DMA((batch + 1,)),
            DMA((batch + 1,)),
            DMA((3, batch)),
            DMA((3, 2, batch)),
        ],
        compiler_params=params(3),
    )(x)


def gathered_layer(residual, pool, table, gate, up, down, shared, score):
    seq_count, batch_count = lax.axis_size("seq"), lax.axis_size("dp")
    devices = seq_count * batch_count
    tokens, width = residual.shape
    own_experts = gate.shape[0] // SPLIT
    room = devices * CAP
    me = lax.axis_index("seq") * batch_count + lax.axis_index("dp")
    mine = (me * own_experts + jnp.arange(own_experts)).astype(jnp.float32)
    named = (table[:, :TOPK, None] == mine).astype(jnp.float32)
    weight = jnp.sum(named * table[:, TOPK:, None], axis=1)
    named = jnp.sum(named, axis=1)
    total = devices * tokens
    order = jnp.arange(total)
    before = (order[None, :] < order[:, None]).astype(jnp.bfloat16)
    rank = jnp.dot(before, named.astype(jnp.bfloat16), preferred_element_type=jnp.float32)
    spot = jnp.where(named > 0, rank, -1.0)
    pick = spot.T[:, None, :] == jnp.arange(room, dtype=jnp.float32)[None, :, None]
    slot_gate = jnp.sum(jnp.where(pick, weight.T[:, None, :], 0.0), axis=-1)
    pick = pick.astype(jnp.bfloat16).reshape(own_experts * room, total)

    pool = pool.reshape(total, width)
    rows = jnp.dot(pick, pool, preferred_element_type=jnp.float32).astype(jnp.bfloat16)
    rows = rows.reshape(own_experts, room, width)
    gate = gate.reshape((own_experts, SPLIT) + gate.shape[1:])
    up = up.reshape((own_experts, SPLIT) + up.shape[1:])
    down = down.reshape((own_experts, SPLIT) + down.shape[1:])
    gate_act = jnp.einsum("ecd,ebdf->ebcf", rows, gate, preferred_element_type=jnp.float32)
    up_act = jnp.einsum("ecd,ebdf->ebcf", rows, up, preferred_element_type=jnp.float32)
    hidden = (jax.nn.silu(gate_act) * up_act).astype(jnp.bfloat16)
    expert_out = jnp.einsum("ebcf,ebfd->ecd", hidden, down, preferred_element_type=jnp.float32)
    expert_out = (expert_out * slot_gate[..., None]).astype(jnp.bfloat16)
    partial = lax.dot_general(
        pick,
        expert_out.reshape(own_experts * room, width),
        (((0,), (0,)), ((), ())),
        preferred_element_type=jnp.float32,
    ).reshape(seq_count, batch_count * tokens, width)
    s = lax.axis_index("seq")
    line = lax.dynamic_slice_in_dim(pool, s * batch_count * tokens, batch_count * tokens)
    share_weight = jax.nn.sigmoid(jnp.dot(line, score, preferred_element_type=jnp.float32))
    shared_part = shared_block(line, *shared) * share_weight[:, None]
    here = (jnp.arange(seq_count) == s)[:, None, None]
    partial = jnp.where(here, partial + shared_part[None], partial).astype(jnp.bfloat16)
    summed = pool_scatter(partial.reshape(devices, tokens, width))
    out = residual.astype(jnp.float32) + summed.astype(jnp.float32)
    return out.astype(jnp.bfloat16)[None]


def body(
    resid,
    queries_keys,
    values,
    doc_ids,
    out_weight,
    norm_gain,
    expert_ids,
    gate_vals,
    expert_gate,
    expert_up,
    expert_down,
    shared_gate,
    shared_up,
    shared_down,
    shared_score,
):
    seq_count = lax.axis_size("seq")
    batch_count = lax.axis_size("dp")
    tokens = resid.shape[1]
    model_width = resid.shape[2]
    local_heads = model_width // HD // seq_count
    dense = expert_gate.shape[0] % SPLIT == 0 and seq_count == 4 and batch_count > 1
    if dense and tokens % 32 == 0:
        table = jnp.concatenate([expert_ids[0].astype(jnp.float32), gate_vals[0]], axis=1)
        table = jnp.pad(table.T, ((0, 0), (0, -tokens % 128)))
        gathered, table = attend_gather(queries_keys[:, 0], values[0], doc_ids[0], table)
        table = table[:, :, :tokens].swapaxes(1, 2).reshape(-1, 2 * TOPK)
        pool, residual = pool_gather(gathered, out_weight, resid[0], norm_gain)
        return gathered_layer(
            residual,
            pool,
            table,
            expert_gate,
            expert_up,
            expert_down,
            (shared_gate, shared_up, shared_down),
            shared_score,
        )
    paired = queries_keys.reshape(2, tokens, seq_count, local_heads, HD)
    valued = values.reshape(1, tokens, seq_count, local_heads, HD)
    documents = doc_ids[0]
    pair_piece = lax.all_to_all(paired, "seq", split_axis=2, concat_axis=1, tiled=True)
    value_piece = lax.all_to_all(valued, "seq", split_axis=2, concat_axis=1, tiled=True)
    attended = attend_heads(
        pair_piece[0, :, 0], pair_piece[1, :, 0], value_piece[0, :, 0], documents
    )
    by_position = attended.reshape(seq_count, tokens, local_heads * HD)
    own_attended = lax.all_to_all(
        by_position, "seq", split_axis=0, concat_axis=2, tiled=True
    ).reshape(tokens, model_width)
    gathered = lax.all_gather(own_attended, "dp", axis=0, tiled=True)
    column_block = jnp.dot(
        gathered,
        out_weight,
        preferred_element_type=jnp.float32,
    ).astype(jnp.bfloat16)
    projected = lax.all_to_all(column_block, "dp", split_axis=0, concat_axis=1, tiled=True)
    residual = (resid[0].astype(jnp.float32) + projected.astype(jnp.float32)).astype(jnp.bfloat16)
    stream = residual.astype(jnp.float32)
    normed = (
        stream * lax.rsqrt(jnp.mean(stream * stream, axis=-1, keepdims=True) + norm_eps) * norm_gain
    ).astype(jnp.bfloat16)
    shared_parts = shared_block(
        lax.all_gather(normed, "dp", axis=0, tiled=True), shared_gate, shared_up, shared_down
    )
    shared_sum = lax.psum_scatter(
        shared_parts.astype(jnp.bfloat16), "dp", scatter_dimension=0, tiled=True
    ).astype(jnp.float32)
    share_weight = jax.nn.sigmoid(jnp.dot(normed, shared_score, preferred_element_type=jnp.float32))
    routes = expert_ids[0]
    route_gates = gate_vals[0]
    slot_ids = slot_numbers(routes)
    slot_range = jnp.arange(EXPERTS * CAP, dtype=jnp.int32)
    picked = jnp.sum(
        (slot_ids[None, :, :] == slot_range[:, None, None]).astype(jnp.int32), axis=-1
    ).astype(jnp.bfloat16)
    buffer = jnp.dot(picked, normed, preferred_element_type=jnp.float32).astype(jnp.bfloat16)
    outgoing = jnp.broadcast_to(
        buffer.reshape(EXPERTS, 1, CAP, model_width), (EXPERTS, SPLIT, CAP, model_width)
    )
    own_pieces = expert_gate.shape[0]
    devices = seq_count * batch_count
    incoming = lax.all_to_all(
        outgoing.reshape(EXPERTS * SPLIT, CAP, model_width),
        ("seq", "dp"),
        split_axis=0,
        concat_axis=0,
        tiled=True,
    )
    results = piece_block(
        incoming.reshape(devices, own_pieces, CAP, model_width), expert_gate, expert_up, expert_down
    )
    returned = lax.all_to_all(
        results.reshape(devices * own_pieces, CAP, model_width),
        ("seq", "dp"),
        split_axis=0,
        concat_axis=0,
        tiled=True,
    )
    expert_out = jnp.sum(
        returned.reshape(EXPERTS, SPLIT, CAP, model_width).astype(jnp.float32), axis=1
    ).reshape(EXPERTS * CAP, model_width)
    fetched = jnp.take(expert_out, slot_ids.reshape(-1), axis=0).reshape(tokens, TOPK, model_width)
    routed = jnp.sum(route_gates[..., None] * fetched, axis=1)
    layer_out = residual.astype(jnp.float32) + routed + share_weight[:, None] * shared_sum
    return layer_out.astype(jnp.bfloat16)[None]


def solution(mesh):
    placed = (
        P(("groups", "dp"), "seq", None),
        P(None, ("groups", "dp"), "seq", None),
        P(("groups", "dp"), "seq", None),
        P(("groups", "dp"), None),
        P(None, "dp"),
        P(),
        P(("groups", "dp"), "seq", None),
        P(("groups", "dp"), "seq", None),
        P(("seq", "dp"), None, None),
        P(("seq", "dp"), None, None),
        P(("seq", "dp"), None, None),
        P(None, "dp"),
        P(None, "dp"),
        P("dp", None),
        P(),
    )
    return jax.shard_map(
        body,
        mesh=mesh,
        in_specs=placed,
        out_specs=P(("groups", "dp"), "seq", None),
        check_vma=False,
    )
```
